32 devices in a mesh: frag: 4 (over y, z), dev: 8 (over x, core).
Axes of the slice: x: 4, y: 2, z: 2, core: 2. Of those that a mesh axis runs over, the one named last changes fastest.
The devices are a block of a 4x4x8 slice.
Arguments:
- a_ints: bfloat16 [416, 104, 104, 104], P(('frag', 'dev')), parts along dimension 0
- c_occ: bfloat16 [416, 32], P('frag'), parts along dimension 0
- c_vir: bfloat16 [416, 64], P('frag'), parts along dimension 0
- eps_occ: float32 [128], P('frag'), parts along dimension 0
- eps_vir: float32 [256], P('frag'), parts along dimension 0
Outputs:
- output: float32 [128, 32], P('frag', 'dev'), parts along dimension 0
There are 4 independent parts. The reference program is written for one: setup_inputs(seed, part) draws one part's arguments, and reference() takes and returns one part's arrays. A program takes and returns all parts, laid end to end along the dimension named above; each array names one.
All inputs are finite; a program needn't handle non-finite values.
Results may differ from the reference program's by a relative error of at most 0.001.
Values are sent between devices in bfloat16 or wider.
A program may use at most 768 MiB of HBM per device.

```python
import jax
import jax.numpy as jnp
from jax import lax

PAD_BASIS = 104
NUM_OCC = 32
NUM_VIRT = 64


def setup_inputs(seed: int = 0, part: int = 0) -> dict:
    key_base = jax.random.fold_in(jax.random.key(seed), part)
    key_ints, key_occ, key_vir, key_eocc, key_evir = jax.random.split(key_base, 5)

    def draw_row(row_idx):
        raw_row = jax.random.normal(jax.random.fold_in(key_ints, row_idx), (PAD_BASIS, PAD_BASIS, PAD_BASIS), jnp.float32)
        mixed_row = (raw_row + 0.5 * jnp.transpose(raw_row, (2, 1, 0))) * (1.25 ** -0.5)
        return mixed_row.astype(jnp.bfloat16)

    a_ints = lax.map(draw_row, jnp.arange(PAD_BASIS))
    c_occ = (jax.random.normal(key_occ, (PAD_BASIS, NUM_OCC), jnp.float32) * PAD_BASIS ** -0.5).astype(jnp.bfloat16)
    c_vir = (jax.random.normal(key_vir, (PAD_BASIS, NUM_VIRT), jnp.float32) * (PAD_BASIS * NUM_VIRT) ** -0.5).astype(jnp.bfloat16)
    eps_occ = jax.random.uniform(key_eocc, (NUM_OCC,), jnp.float32, -1.5, -0.5)
    eps_vir = jax.random.uniform(key_evir, (NUM_VIRT,), jnp.float32, 0.3, 2.0)
    return {"a_ints": a_ints, "c_occ": c_occ, "c_vir": c_vir, "eps_occ": eps_occ, "eps_vir": eps_vir}


def reference(a_ints, c_occ, c_vir, eps_occ, eps_vir):
    occ_32 = c_occ.astype(jnp.float32)
    vir_32 = c_vir.astype(jnp.float32)

    def first_half(a_row):
        t_one = jnp.einsum("qrs,rj->qsj", a_row.astype(jnp.float32), occ_32).astype(jnp.bfloat16)
        return jnp.einsum("qsj,sb->qjb", t_one.astype(jnp.float32), vir_32).astype(jnp.bfloat16)

    half_mo = lax.map(first_half, a_ints)
    g_mat = jnp.einsum("pqjb,qa->pjba", half_mo.astype(jnp.float32), vir_32).astype(jnp.bfloat16)
    v_mo = jnp.einsum("pjba,pi->jbai", g_mat.astype(jnp.float32), occ_32)
    v_swap = jnp.swapaxes(v_mo, 1, 2)
    denominator = (eps_occ[:, None, None, None] + eps_occ[None, None, None, :]
                   - eps_vir[None, :, None, None] - eps_vir[None, None, :, None])
    pair_ji = jnp.sum(v_mo * (2.0 * v_mo - v_swap) / denominator, axis=(1, 2))
    return pair_ji.T
```

```python
import functools

import jax
import jax.numpy as jnp
from jax import lax
from jax.experimental import pallas as pl
from jax.experimental.pallas import tpu as pltpu
from jax.sharding import PartitionSpec as P

MESH = pl.DeviceIdType.MESH
LANES = 128
SUB = 16
F32, BF16 = jnp.float32, jnp.bfloat16


def dot(lhs, rhs):
    return jnp.dot(lhs, rhs, preferred_element_type=F32)


def groups_of(ends):
    starts = [0] + [e + 1 for e in ends[:-1]]
    return [(s, e - s + 1) for s, e in zip(starts, ends)]


def kernel(dims, a_hbm, cot_hbm, cvt_hbm, eo_hbm, ev_hbm, out_ref, abuf, cot, cvt, eo, ev, wv, tbuf, gsend, grecv, kron, vbuf, wbuf, ebuf,
           a_sem, c_sem, send_sem, recv_sem):
    rows, n, o, v, size, slots, units, groups = dims
    me, frag = lax.axis_index("dev"), lax.axis_index("frag")
    chips = size // 2
    chip, core = me // 2, me % 2
    pair = 2 * v
    od = o // size

    def peer(dx, dc):
        return lax.rem(chip + dx, chips) * 2 + lax.rem(core + dc, 2)

    relations = [(dx, dc) for dx in sorted(range(chips), key=lambda d: -min(d, chips - d)) for dc in range(2) if (dx, dc) != (0, 0)]

    barrier = pltpu.get_barrier_semaphore()
    for dx, dc in relations:
        pl.semaphore_signal(barrier, inc=1, device_id=(frag, peer(dx, dc)), device_id_type=MESH)

    small = [pltpu.make_async_copy(src, dst, c_sem.at[k]) for k, (src, dst) in enumerate([(cot_hbm, cot), (cvt_hbm, cvt), (eo_hbm, eo), (ev_hbm, ev)])]
    for copy in small:
        copy.start()

    def load(p):
        slot = lax.rem(p, slots)
        return pltpu.make_async_copy(a_hbm.at[p], abuf.at[slot], a_sem.at[slot])

    for p in range(min(slots, rows)):
        load(p).start()
    for copy in small:
        copy.wait()

    cv = jnp.pad(cvt[...].astype(F32), ((0, 0), (0, LANES - n))).T.astype(BF16)
    zero = jnp.zeros_like(cv)
    wv[...] = jnp.concatenate([jnp.concatenate([cv, zero], 1), jnp.concatenate([zero, cv], 1)], 0)

    def share(unit, group, rel):
        start, count = groups[unit][group]
        target = peer(*relations[rel])
        return pltpu.make_async_remote_copy(
            src_ref=gsend.at[target, unit, pl.ds(start, count)],
            dst_ref=grecv.at[unit, pl.ds(me * rows + start, count)],
            send_sem=send_sem.at[unit, group, rel],
            recv_sem=recv_sem.at[unit, group, rel],
            device_id=(frag, target),
            device_id_type=MESH,
        )

    def first_half(p, carry):
        slot = lax.rem(p, slots)
        load(p).wait()
        lhs = cot[...]
        fill = jnp.zeros((n, LANES - n), BF16)
        for q in range(0, n, 2):
            rhs = jnp.concatenate([abuf[slot, q], fill, abuf[slot, q + 1], fill], 1)
            t = dot(lhs, rhs)
            tbuf[pl.ds(q, o, stride=n), :] = t[:, :LANES]
            tbuf[pl.ds(q + 1, o, stride=n), :] = t[:, LANES:]

        @pl.when(p + slots < rows)
        def _():
            load(p + slots).start()

        weights = wv[...]
        for d in range(size):
            halves = []
            for u in range(units):
                j = d * od + 2 * u
                t2 = jnp.concatenate([tbuf[j * n:(j + 1) * n, :], tbuf[(j + 1) * n:(j + 2) * n, :]], 1).astype(BF16)
                halves.append(dot(t2, weights).astype(BF16))
            g = dot(cvt[...], jnp.concatenate(halves, 1)).astype(BF16)
            for u in range(units):
                gsend[d, u, p] = g[:, u * pair:(u + 1) * pair]

        for group, (start, count) in enumerate(groups[0]):
            @pl.when(p == start + count - 1)
            def _(group=group):
                if group == 0:
                    pl.semaphore_wait(barrier, len(relations))
                for rel in range(len(relations)):
                    share(0, group, rel).start()
        return carry

    lax.fori_loop(0, rows, first_half, 0)
    for unit in range(1, units):
        for group in range(len(groups[unit])):
            for rel in range(len(relations)):
                share(unit, group, rel).start()

    total = size * rows
    spread_i = (lax.broadcasted_iota(jnp.int32, (o * SUB, o), 0) // SUB == lax.broadcasted_iota(jnp.int32, (o * SUB, o), 1)).astype(F32).astype(BF16)
    by_p = dot(spread_i, cot[...]).astype(BF16)
    step = LANES * 2
    for start in range(0, total * SUB, step):
        width = min(step, total * SUB - start)
        spread_p = (lax.broadcasted_iota(jnp.int32, (total, width), 0)
                    == (lax.broadcasted_iota(jnp.int32, (total, width), 1) + start) // SUB).astype(F32).astype(BF16)
        same = (lax.broadcasted_iota(jnp.int32, (o * SUB, width), 0) % SUB == lax.broadcasted_iota(jnp.int32, (o * SUB, width), 1) % SUB)
        kron[:, start:start + width] = jnp.where(same, dot(by_p, spread_p), 0.0).astype(BF16)

    own = pl.ds(me * rows, rows)
    for unit in range(units):
        grecv[unit, own] = gsend[me, unit]

    ev_row, eo_row = ev[...], eo[...]
    diag = lax.broadcasted_iota(jnp.int32, (v, v), 0) == lax.broadcasted_iota(jnp.int32, (v, v), 1)
    ev_col = jnp.sum(jnp.where(diag, jnp.broadcast_to(ev_row, (v, v)), 0.0), 1, keepdims=True)
    at = lax.broadcasted_iota(jnp.int32, (1, o), 1)
    diag_o = lax.broadcasted_iota(jnp.int32, (o, o), 0) == lax.broadcasted_iota(jnp.int32, (o, o), 1)
    eo_col = jnp.sum(jnp.where(diag_o, jnp.broadcast_to(eo_row, (o, o)), 0.0), 1, keepdims=True)
    left = lax.broadcasted_iota(jnp.int32, (v, pair), 1) < v

    def energies(unit):
        energy_j = [jnp.sum(jnp.where(at == me * od + 2 * unit + h, eo_row, 0.0), 1, keepdims=True) for h in range(2)]
        base = jnp.concatenate([e - ev_row for e in energy_j], 1) - ev_col
        for i in range(o):
            wbuf[i] = 1.0 / (eo_col[i:i + 1, :] + base)

        for group in range(len(groups[unit])):
            for rel in range(len(relations)):
                share(unit, group, rel).wait_recv()

        for block in range(0, v, 2 * SUB):
            rhs = jnp.concatenate([grecv[unit, :, block + k * SUB:block + (k + 1) * SUB, :].reshape(total * SUB, pair) for k in range(2)], 1)
            part = dot(kron[...], rhs)
            for k in range(2):
                vbuf[:, block + k * SUB:block + (k + 1) * SUB, :] = part[:, k * pair:(k + 1) * pair].reshape(o, SUB, pair)

        for i in range(0, o, 2):
            x = vbuf[i:i + 2].reshape(2 * v, pair)
            xt = x.T
            turned = pltpu.roll(xt, v, 1)
            top = jnp.where(left, xt[:v], turned[v:])
            bottom = jnp.where(left, turned[:v], xt[v:])
            for k, swap in enumerate((top, bottom)):
                own_v = x[k * v:(k + 1) * v]
                ebuf[i + k:i + k + 1, :] = jnp.sum(own_v * (2.0 * own_v - swap) * wbuf[i + k], 0, keepdims=True)
        sums = ebuf[...]
        return [jnp.sum(sums[:, h * v:(h + 1) * v], 1, keepdims=True) for h in range(2)]

    columns = []
    for unit in range(units):
        columns += energies(unit)
    out_ref[...] = jnp.concatenate(columns, 1)

    for unit in range(units):
        for group in range(len(groups[unit])):
            for rel in range(len(relations)):
                share(unit, group, rel).wait_send()


def solution(mesh):
    size = mesh.shape["dev"]

    def per_device(a_ints, c_occ, c_vir, eps_occ, eps_vir):
        rows, n = a_ints.shape[0], a_ints.shape[1]
        o, v = c_occ.shape[1], c_vir.shape[1]
        units = o // size // 2
        slots = 4
        early = [e for e in (0, 2, 4, 8) if e < rows - 1] + [rows - 1]
        groups = [groups_of(early)] + [[(0, rows)]] * (units - 1)
        most = max(len(g) for g in groups)
        dims = (rows, n, o, v, size, slots, units, groups)
        any_spec = pl.BlockSpec(memory_space=pl.ANY)
        return pl.pallas_call(
            functools.partial(kernel, dims),
            out_shape=jax.ShapeDtypeStruct((o, o // size), F32),
            in_specs=[any_spec] * 5,
            out_specs=pl.BlockSpec(memory_space=pltpu.VMEM),
            scratch_shapes=[
                pltpu.VMEM((slots, n, n, n), BF16),
                pltpu.VMEM((o, n), BF16),
                pltpu.VMEM((v, n), BF16),
                pltpu.VMEM((1, o), F32),
                pltpu.VMEM((1, v), F32),
                pltpu.VMEM((2 * LANES, 2 * v), BF16),
                pltpu.VMEM((o * n, LANES), F32),
                pltpu.VMEM((size, units, rows, v, 2 * v), BF16),
                pltpu.VMEM((units, size * rows, v, 2 * v), BF16),
                pltpu.VMEM((o * SUB, size * rows * SUB), BF16),
                pltpu.VMEM((o, v, 2 * v), F32),
                pltpu.VMEM((o, v, 2 * v), F32),
                pltpu.VMEM((o, 2 * v), F32),
                pltpu.SemaphoreType.DMA((slots,)),
                pltpu.SemaphoreType.DMA((4,)),
                pltpu.SemaphoreType.DMA((units, most, size - 1)),
                pltpu.SemaphoreType.DMA((units, most, size - 1)),
            ],
            compiler_params=pltpu.CompilerParams(collective_id=0, has_side_effects=True, vmem_limit_bytes=62 * 2**20),
        )(a_ints, c_occ.T, c_vir.T, eps_occ.reshape(1, o), eps_vir.reshape(1, v))

    return jax.shard_map(
        per_device,
        mesh=mesh,
        in_specs=(P(("frag", "dev")), P("frag"), P("frag"), P("frag"), P("frag")),
        out_specs=P("frag", "dev"),
        check_vma=False,
    )
```

```python
import functools

import jax
import jax.numpy as jnp
from jax import lax
from jax.experimental import pallas as pl
from jax.experimental.pallas import tpu as pltpu
from jax.sharding import PartitionSpec as P

MESH = pl.DeviceIdType.MESH
LANES = 128
SUB = 16
F32, BF16 = jnp.float32, jnp.bfloat16


def dot(lhs, rhs):
    return jnp.dot(lhs, rhs, preferred_element_type=F32)


def on(condition, action):
    if isinstance(condition, bool):
        if condition:
            action()
    else:
        pl.when(condition)(action)


def kernel(dims, a_hbm, cot_hbm, cvt_hbm, eo_hbm, ev_hbm, out_ref, abuf, cot, cvt, eo, ev, lhs, wv, tbuf, hbuf, gsend, grecv, kron, vbuf, wbuf, ebuf,
           a_sem, first_sem, c_sem, send_sem, recv_sem):
    rows, n, o, v, size, slots, units, groups, parts = dims
    me, frag = lax.axis_index("dev"), lax.axis_index("frag")
    chips = size // 2
    chip, core = me // 2, me % 2
    pair = 2 * v
    od = o // size
    total = size * rows
    starts = [sum(groups[:g]) for g in range(len(groups))]

    def peer(dx, dc):
        return lax.rem(chip + dx, chips) * 2 + lax.rem(core + dc, 2)

    relations = [(dx, dc) for dx in sorted(range(chips), key=lambda d: -min(d, chips - d)) for dc in range(2) if (dx, dc) != (0, 0)]

    def load(p):
        slot = lax.rem(p, slots)
        return pltpu.make_async_copy(a_hbm.at[p], abuf.at[slot], a_sem.at[slot])

    small = [pltpu.make_async_copy(src, dst, c_sem.at[k]) for k, (src, dst) in enumerate([(cot_hbm, cot), (cvt_hbm, cvt), (eo_hbm, eo), (ev_hbm, ev)])]
    cuts = [n * k // parts // 2 * 2 for k in range(parts)] + [n]
    opening = [pltpu.make_async_copy(a_hbm.at[0, pl.ds(x, y - x)], abuf.at[0, pl.ds(x, y - x)], first_sem.at[k])
               for k, (x, y) in enumerate(zip(cuts, cuts[1:]))]
    small[0].start()
    opening[0].start()
    small[1].start()
    for copy in opening[1:]:
        copy.start()
    for p in range(1, min(slots, rows)):
        load(p).start()
    small[2].start()
    small[3].start()
    barrier = pltpu.get_barrier_semaphore()
    for dx, dc in relations:
        pl.semaphore_signal(barrier, inc=1, device_id=(frag, peer(dx, dc)), device_id_type=MESH)

    with jax.named_scope("waitC"):
        small[0].wait()
    row, col = lax.broadcasted_iota(jnp.int32, (o, o), 0), lax.broadcasted_iota(jnp.int32, (o, o), 1)
    order = (col == 2 * lax.rem(row, o // 2) + row // (o // 2)).astype(F32).astype(BF16)
    lhs[...] = dot(order, cot[...]).astype(BF16)
    def share(unit, group, rel):
        start, count = starts[group], groups[group]
        target = peer(*relations[rel])
        return pltpu.make_async_remote_copy(
            src_ref=gsend.at[target, unit, pl.ds(start, count)],
            dst_ref=grecv.at[unit, pl.ds(size * start + me * count, count)],
            send_sem=send_sem.at[unit, group, rel],
            recv_sem=recv_sem.at[unit, group, rel],
            device_id=(frag, target),
            device_id_type=MESH,
        )

    def occupied(slot, first, last):
        fill = jnp.zeros((n, LANES - n), BF16)
        for q in range(first, last, 2):
            rhs = jnp.concatenate([abuf[slot, q], fill, abuf[slot, q + 1], fill], 1)
            t = dot(lhs[...], rhs)
            tbuf[pl.ds(q, o, stride=n), :] = t[:, :LANES]
            tbuf[pl.ds(q + 1, o, stride=n), :] = t[:, LANES:]

    def first_half(p, carry):
        slot = lax.rem(p, slots)
        if isinstance(p, int):
            for k, copy in enumerate(opening):
                with jax.named_scope("waitA"):
                    copy.wait()
                if k == parts - 1:
                    small[1].wait()
                    cv = jnp.pad(cvt[...].astype(F32), ((0, 0), (0, LANES - n))).T.astype(BF16)
                    zero = jnp.zeros_like(cv)
                    wv[...] = jnp.concatenate([jnp.concatenate([cv, zero], 1), jnp.concatenate([zero, cv], 1)], 0)
                with jax.named_scope("step1"):
                    occupied(0, cuts[k], cuts[k + 1])
        else:
            with jax.named_scope("waitA"):
                load(p).wait()
            with jax.named_scope("step1"):
                occupied(slot, 0, n)

        def refill():
            load(p + slots).start()

        on(p + slots < rows, refill)

        half = o // 2 * n
        with jax.named_scope("step2"):
            hbuf[...] = dot(jnp.concatenate([tbuf[:half, :], tbuf[half:, :]], 1).astype(BF16), wv[...])
        with jax.named_scope("step3"):
            for d in range(size):
                at = [d * units + u for u in range(units)]
                h = jnp.concatenate([hbuf[k * n:(k + 1) * n, :] for k in at], 1).astype(BF16)
                g = dot(cvt[...], h).astype(BF16)
                for u in range(units):
                    gsend[d, u, p] = g[:, u * pair:(u + 1) * pair]

        for group, (start, count) in enumerate(zip(starts, groups)):
            def send(group=group):
                if group == 0:
                    with jax.named_scope("waitB"):
                        pl.semaphore_wait(barrier, len(relations))
                for unit in range(1 if group == 0 else units):
                    for rel in range(len(relations)):
                        share(unit, group, rel).start()

            on(p == start + count - 1, send)
        return carry

    first_half(0, 0)
    lax.fori_loop(1, rows, first_half, 0)
    for unit in range(1, units):
        for rel in range(len(relations)):
            share(unit, 0, rel).start()

    small[2].wait()
    small[3].wait()
    with jax.named_scope("kron"):
        spread_i = (lax.broadcasted_iota(jnp.int32, (o * SUB, o), 0) // SUB == lax.broadcasted_iota(jnp.int32, (o * SUB, o), 1)).astype(F32).astype(BF16)
        by_p = dot(spread_i, cot[...]).astype(BF16)
        for start, count in zip(starts, groups):
            for at in range(size * start * SUB, size * (start + count) * SUB, 2 * LANES):
                width = min(2 * LANES, size * (start + count) * SUB - at)
                place = (lax.broadcasted_iota(jnp.int32, (total, width), 1) + at) // SUB - size * start
                spread_p = (lax.broadcasted_iota(jnp.int32, (total, width), 0) == place // count * rows + start + place % count).astype(F32).astype(BF16)
                same = (lax.broadcasted_iota(jnp.int32, (o * SUB, width), 0) % SUB == lax.broadcasted_iota(jnp.int32, (o * SUB, width), 1) % SUB)
                kron[:, at:at + width] = jnp.where(same, dot(by_p, spread_p), 0.0).astype(BF16)

    for unit in range(units):
        for start, count in zip(starts, groups):
            grecv[unit, pl.ds(size * start + me * count, count)] = gsend[me, unit, start:start + count]

    ev_row, eo_row = ev[...], eo[...]
    diag = lax.broadcasted_iota(jnp.int32, (v, v), 0) == lax.broadcasted_iota(jnp.int32, (v, v), 1)
    ev_col = jnp.sum(jnp.where(diag, jnp.broadcast_to(ev_row, (v, v)), 0.0), 1, keepdims=True)
    eo_col = jnp.sum(jnp.where(row == col, jnp.broadcast_to(eo_row, (o, o)), 0.0), 1, keepdims=True)
    left = lax.broadcasted_iota(jnp.int32, (v, pair), 1) < v

    def integrals(unit, first, last, add):
        width = (last - first) * SUB
        for block in range(0, v, 2 * SUB):
            rhs = jnp.concatenate([grecv[unit, first:last, block + k * SUB:block + (k + 1) * SUB, :].reshape(width, pair) for k in range(2)], 1)
            part = dot(kron[:, first * SUB:last * SUB], rhs)
            for k in range(2):
                at = slice(block + k * SUB, block + (k + 1) * SUB)
                new = part[:, k * pair:(k + 1) * pair].reshape(o, SUB, pair)
                vbuf[:, at, :] = vbuf[:, at, :] + new if add else new

    def energies(unit):
        with jax.named_scope("W"):
            energy_j = [jnp.sum(jnp.where(lax.broadcasted_iota(jnp.int32, (1, o), 1) == me * od + 2 * unit + h, eo_row, 0.0), 1, keepdims=True) for h in range(2)]
            base = jnp.concatenate([e - ev_row for e in energy_j], 1) - ev_col
            for i in range(o):
                wbuf[i] = 1.0 / (eo_col[i:i + 1, :] + base)

        with jax.named_scope("waitR"):
            for group in range(1, len(groups)):
                for rel in range(len(relations)):
                    share(unit, group, rel).wait_recv()
        with jax.named_scope("V"):
            integrals(unit, size * starts[1], total, False)
        with jax.named_scope("waitR0"):
            for rel in range(len(relations)):
                share(unit, 0, rel).wait_recv()
        with jax.named_scope("V0"):
            integrals(unit, 0, size * starts[1], True)

        with jax.named_scope("E"):
            for i in range(0, o, 2):
                x = vbuf[i:i + 2].reshape(2 * v, pair)
                xt = x.T
                turned = pltpu.roll(xt, v, 1)
                top = jnp.where(left, xt[:v], turned[v:])
                bottom = jnp.where(left, turned[:v], xt[v:])
                for k, swap in enumerate((top, bottom)):
                    own_v = x[k * v:(k + 1) * v]
                    ebuf[i + k:i + k + 1, :] = jnp.sum(own_v * (2.0 * own_v - swap) * wbuf[i + k], 0, keepdims=True)
        with jax.named_scope("sum"):
            sums = ebuf[...].T
            return [jnp.sum(sums[h * v:(h + 1) * v], 0, keepdims=True) for h in range(2)]

    pairs = []
    for unit in range(units):
        pairs += energies(unit)
    out_ref[...] = jnp.concatenate(pairs, 0)

    with jax.named_scope("waitS"):
        for unit in range(units):
            for group in range(len(groups)):
                for rel in range(len(relations)):
                    share(unit, group, rel).wait_send()


def solution(mesh):
    size = mesh.shape["dev"]

    def per_device(a_ints, c_occ, c_vir, eps_occ, eps_vir):
        rows, n = a_ints.shape[0], a_ints.shape[1]
        o, v = c_occ.shape[1], c_vir.shape[1]
        units = o // size // 2
        slots = 4
        groups = [g for g in (1, 1, 2, 4) if g < rows]
        while sum(groups) >= rows:
            groups.pop()
        groups.append(rows - sum(groups))
        parts = 4
        dims = (rows, n, o, v, size, slots, units, tuple(groups), parts)
        any_spec = pl.BlockSpec(memory_space=pl.ANY)
        return pl.pallas_call(
            functools.partial(kernel, dims),
            out_shape=pltpu.VMEM((o // size, o), F32),
            in_specs=[any_spec] * 5,
            out_specs=pl.BlockSpec(memory_space=pltpu.VMEM),
            scratch_shapes=[
                pltpu.VMEM((slots, n, n, n), BF16),
                pltpu.VMEM((o, n), BF16),
                pltpu.VMEM((v, n), BF16),
                pltpu.VMEM((1, o), F32),
                pltpu.VMEM((1, v), F32),
                pltpu.VMEM((o, n), BF16),
                pltpu.VMEM((2 * LANES, 2 * v), BF16),
                pltpu.VMEM((o * n, LANES), F32),
                pltpu.VMEM((o // 2 * n, 2 * v), F32),
                pltpu.VMEM((size, units, rows, v, 2 * v), BF16),
                pltpu.VMEM((units, size * rows, v, 2 * v), BF16),
                pltpu.VMEM((o * SUB, size * rows * SUB), BF16),
                pltpu.VMEM((o, v, 2 * v), F32),
                pltpu.VMEM((o, v, 2 * v), F32),
                pltpu.VMEM((o, 2 * v), F32),
                pltpu.SemaphoreType.DMA((slots,)),
                pltpu.SemaphoreType.DMA((parts,)),
                pltpu.SemaphoreType.DMA((4,)),
                pltpu.SemaphoreType.DMA((units, len(groups), size - 1)),
                pltpu.SemaphoreType.DMA((units, len(groups), size - 1)),
            ],
            compiler_params=pltpu.CompilerParams(collective_id=0, has_side_effects=True, vmem_limit_bytes=62 * 2**20),
        )(a_ints, c_occ.T, c_vir.T, eps_occ.reshape(1, o), eps_vir.reshape(1, v)).T

    return jax.shard_map(
        per_device,
        mesh=mesh,
        in_specs=(P(("frag", "dev")), P("frag"), P("frag"), P("frag"), P("frag")),
        out_specs=P("frag", "dev"),
        check_vma=False,
    )
```

```python
import functools

import jax
import jax.numpy as jnp
from jax import lax
from jax.experimental import pallas as pl
from jax.experimental.pallas import tpu as pltpu
from jax.sharding import PartitionSpec as P

MESH = pl.DeviceIdType.MESH
LANES = 128
SUB = 16
F32, BF16 = jnp.float32, jnp.bfloat16


def dot(lhs, rhs):
    return jnp.dot(lhs, rhs, preferred_element_type=F32)


def iota(shape, dim):
    return lax.broadcasted_iota(jnp.int32, shape, dim)


def one_hot(mask):
    return mask.astype(F32).astype(BF16)


def kernel(dims, a_hbm, cot_hbm, cvt_hbm, eo_hbm, ev_hbm, out_ref, abuf, cot, cvt, eo, ev, lhs, wv, tbuf, hbuf, gsend, grecv, kron, vbuf, wbuf, ebuf,
           a_sem, first_sem, c_sem, send_sem, recv_sem):
    rows, n, o, v, size, slots, units, groups, joint, parts = dims
    me, frag = lax.axis_index("dev"), lax.axis_index("frag")
    chips = size // 2
    chip, core = me // 2, me % 2
    pair = 2 * v
    od = o // size
    total = size * rows
    starts = [sum(groups[:g]) for g in range(len(groups))]
    last = len(groups) - 1

    def peer(dx, dc):
        return lax.rem(chip + dx, chips) * 2 + lax.rem(core + dc, 2)

    relations = [(dx, dc) for dx in sorted(range(chips), key=lambda d: -min(d, chips - d)) for dc in range(2) if (dx, dc) != (0, 0)]

    def load(p):
        slot = lax.rem(p, slots)
        return pltpu.make_async_copy(a_hbm.at[p], abuf.at[slot], a_sem.at[slot])

    small = [pltpu.make_async_copy(src, dst, c_sem.at[k]) for k, (src, dst) in enumerate([(cot_hbm, cot), (cvt_hbm, cvt), (eo_hbm, eo), (ev_hbm, ev)])]
    cuts = [0, n * 9 // 16 // 2 * 2, n]
    opening = [pltpu.make_async_copy(a_hbm.at[0, pl.ds(x, y - x)], abuf.at[0, pl.ds(x, y - x)], first_sem.at[k])
               for k, (x, y) in enumerate(zip(cuts, cuts[1:]))]
    small[0].start()
    small[1].start()
    for copy in opening:
        copy.start()
    barrier = pltpu.get_barrier_semaphore()
    for dx, dc in relations:
        pl.semaphore_signal(barrier, inc=1, device_id=(frag, peer(dx, dc)), device_id_type=MESH)

    with jax.named_scope("waitC"):
        small[0].wait()
        small[1].wait()
    for p in range(1, min(slots, rows)):
        load(p).start()
    small[2].start()
    small[3].start()
    row, col = iota((o, o), 0), iota((o, o), 1)
    lhs[...] = dot(one_hot(col == lax.rem(row, size) * od + row // (2 * size) * 2 + lax.rem(row // size, 2)), cot[...]).astype(BF16)
    cv = jnp.pad(cvt[...].astype(F32), ((0, 0), (0, LANES - n))).T.astype(BF16)
    zero = jnp.zeros_like(cv)
    wv[...] = jnp.concatenate([jnp.concatenate([cv, zero], 1), jnp.concatenate([zero, cv], 1)], 0)

    def share(which, group, rel, sem):
        start, count = starts[group], groups[group]
        target = peer(*relations[rel])
        return pltpu.make_async_remote_copy(
            src_ref=gsend.at[target, which, pl.ds(start, count)],
            dst_ref=grecv.at[which, pl.ds(size * start + me * count, count)],
            send_sem=send_sem,
            recv_sem=recv_sem.at[sem],
            device_id=(frag, target),
            device_id_type=MESH,
        )

    def arrivals(which, count, sem):
        part = grecv.at[which, pl.ds(0, (size - 1) * count)]
        return pltpu.make_async_remote_copy(
            src_ref=part, dst_ref=part, send_sem=send_sem, recv_sem=recv_sem.at[sem], device_id=(frag, peer(*relations[0])), device_id_type=MESH)

    every, first_unit, other_units = pl.ds(0, units), pl.ds(0, 1), pl.ds(1, units - 1)

    def send(which, group, sem):
        for rel in range(len(relations)):
            share(which, group, rel, sem).start()

    def occupied(slot, first, end):
        fill = jnp.zeros((n, LANES - n), BF16)
        for q in range(first, end, 2):
            t = dot(lhs[...], jnp.concatenate([abuf[slot, q], fill, abuf[slot, q + 1], fill], 1))
            tbuf[pl.ds(q, o, stride=n), :] = t[:, :LANES]
            tbuf[pl.ds(q + 1, o, stride=n), :] = t[:, LANES:]

    depth = size * n

    def half_mo(unit, first, end):
        even, odd = (tbuf[(2 * unit + k) * depth + first:(2 * unit + k) * depth + end, :] for k in range(2))
        return dot(jnp.concatenate([even, odd], 1).astype(BF16), wv[...])

    def virtual(unit, p):
        with jax.named_scope("step3"):
            for d in range(0, size, 2):
                h = jnp.concatenate([hbuf[unit * depth + k * n:unit * depth + (k + 1) * n, :] for k in (d, d + 1)], 1)
                g = dot(cvt[...], h.astype(BF16)).astype(BF16)
                for k in range(2):
                    gsend[d + k, unit, p] = g[:, k * pair:(k + 1) * pair]

    def open_row():
        for k, copy in enumerate(opening):
            with jax.named_scope("waitA"):
                copy.wait()
            with jax.named_scope("step1"):
                occupied(0, cuts[k], cuts[k + 1])
        if slots < rows:
            load(slots).start()
        for unit in range(units):
            with jax.named_scope("step2"):
                for k in range(2):
                    at = k * depth // 2
                    hbuf[unit * depth + at:unit * depth + at + depth // 2, :] = half_mo(unit, at, at + depth // 2)
            virtual(unit, 0)
            if unit == 0:
                with jax.named_scope("waitB"):
                    pl.semaphore_wait(barrier, len(relations))
            send(pl.ds(unit, 1), 0, 0)

    def next_row(p, carry):
        slot = lax.rem(p, slots)
        with jax.named_scope("waitA"):
            load(p).wait()
        with jax.named_scope("step1"):
            occupied(slot, 0, n)

        @pl.when(p + slots < rows)
        def _():
            load(p + slots).start()

        with jax.named_scope("step2"):
            for unit in range(units):
                hbuf[unit * depth:(unit + 1) * depth, :] = half_mo(unit, 0, depth)
        for unit in range(units):
            virtual(unit, p)
        for group in range(1, len(groups)):
            @pl.when(p == starts[group] + groups[group] - 1)
            def _(group=group):
                if group < joint:
                    send(every, group, 0)
                else:
                    send(first_unit, group, 1)
        return carry

    open_row()
    lax.fori_loop(1, rows, next_row, 0)
    for group in range(joint, len(groups)):
        send(other_units, group, 2 + group - joint)

    small[2].wait()
    small[3].wait()
    with jax.named_scope("kron"):
        by_p = dot(one_hot(iota((o * SUB, o), 0) // SUB == iota((o * SUB, o), 1)), cot[...]).astype(BF16)
        for start, count in zip(starts, groups):
            for at in range(size * start * SUB, size * (start + count) * SUB, 2 * LANES):
                width = min(2 * LANES, size * (start + count) * SUB - at)
                place = (iota((total, width), 1) + at) // SUB - size * start
                spread_p = one_hot(iota((total, width), 0) == place // count * rows + start + place % count)
                same = iota((o * SUB, width), 0) % SUB == iota((o * SUB, width), 1) % SUB
                kron[:, at:at + width] = jnp.where(same, dot(by_p, spread_p), 0.0).astype(BF16)

    for unit in range(units):
        for start, count in zip(starts, groups):
            grecv[unit, pl.ds(size * start + me * count, count)] = gsend[me, unit, start:start + count]

    ev_row, eo_row = ev[...], eo[...]
    diag = iota((v, v), 0) == iota((v, v), 1)
    ev_col = jnp.sum(jnp.where(diag, jnp.broadcast_to(ev_row, (v, v)), 0.0), 1, keepdims=True)
    eo_col = jnp.sum(jnp.where(row == col, jnp.broadcast_to(eo_row, (o, o)), 0.0), 1, keepdims=True)
    left = iota((v, pair), 1) < v

    def weights(unit):
        with jax.named_scope("W"):
            energy_j = [jnp.sum(jnp.where(iota((1, o), 1) == me * od + 2 * unit + h, eo_row, 0.0), 1, keepdims=True) for h in range(2)]
            base = jnp.concatenate([e - ev_row for e in energy_j], 1) - ev_col
            for i in range(o):
                wbuf[i] = 1.0 / (eo_col[i:i + 1, :] + base)

    def integrals(unit, first, end, add):
        with jax.named_scope("V"):
            width = (end - first) * SUB
            for block in range(0, v, 2 * SUB):
                rhs = jnp.concatenate([grecv[unit, first:end, block + k * SUB:block + (k + 1) * SUB, :].reshape(width, pair) for k in range(2)], 1)
                part = dot(kron[:, first * SUB:end * SUB], rhs)
                for k in range(2):
                    at = slice(block + k * SUB, block + (k + 1) * SUB)
                    new = part[:, k * pair:(k + 1) * pair].reshape(o, SUB, pair)
                    vbuf[:, at, :] = vbuf[:, at, :] + new if add else new

    def energies():
        with jax.named_scope("E"):
            for i in range(0, o, 2):
                x = vbuf[i:i + 2].reshape(2 * v, pair)
                xt = x.T
                turned = pltpu.roll(xt, v, 1)
                top = jnp.where(left, xt[:v], turned[v:])
                bottom = jnp.where(left, turned[:v], xt[v:])
                for k, swap in enumerate((top, bottom)):
                    own = x[k * v:(k + 1) * v]
                    ebuf[i + k:i + k + 1, :] = jnp.sum(own * (2.0 * own - swap) * wbuf[i + k], 0, keepdims=True)

    def totals():
        with jax.named_scope("sum"):
            sums = ebuf[...].T
            return [jnp.sum(sums[h * v:(h + 1) * v], 0, keepdims=True) for h in range(2)]

    pairs = []
    for unit in range(units):
        weights(unit)
        if unit == 0:
            with jax.named_scope("waitR"):
                arrivals(every, starts[joint], 0).wait_recv()
                arrivals(first_unit, rows - starts[joint], 1).wait_recv()
            integrals(unit, 0, total, False)
        else:
            for group in range(joint, len(groups)):
                if unit == 1:
                    with jax.named_scope(f"waitR{group}"):
                        arrivals(other_units, groups[group], 2 + group - joint).wait_recv()
                first = group == joint
                integrals(unit, 0 if first else size * starts[group], size * (starts[group] + groups[group]), not first)
        energies()
        pairs += totals()
    out_ref[...] = jnp.concatenate(pairs, 0)

    sent = gsend.at[pl.ds(0, size - 1)]
    with jax.named_scope("waitS"):
        pltpu.make_async_remote_copy(
            src_ref=sent, dst_ref=sent, send_sem=send_sem, recv_sem=recv_sem.at[0], device_id=(frag, peer(*relations[0])), device_id_type=MESH).wait_send()


def solution(mesh):
    size = mesh.shape["dev"]

    def per_device(a_ints, c_occ, c_vir, eps_occ, eps_vir):
        rows, n = a_ints.shape[0], a_ints.shape[1]
        o, v = c_occ.shape[1], c_vir.shape[1]
        units = o // size // 2
        slots, parts = 4, 2
        groups = (1, 1, 2, rows - 8, 2, 2)
        joint = 3
        dims = (rows, n, o, v, size, slots, units, groups, joint, parts)
        any_spec = pl.BlockSpec(memory_space=pl.ANY)
        return pl.pallas_call(
            functools.partial(kernel, dims),
            out_shape=pltpu.VMEM((o // size, o), F32),
            in_specs=[any_spec] * 5,
            out_specs=pl.BlockSpec(memory_space=pltpu.VMEM),
            scratch_shapes=[
                pltpu.VMEM((slots, n, n, n), BF16),
                pltpu.VMEM((o, n), BF16),
                pltpu.VMEM((v, n), BF16),
                pltpu.VMEM((1, o), F32),
                pltpu.VMEM((1, v), F32),
                pltpu.VMEM((o, n), BF16),
                pltpu.VMEM((2 * LANES, 2 * v), BF16),
                pltpu.VMEM((o * n, LANES), F32),
                pltpu.VMEM((units * size * n, 2 * v), F32),
                pltpu.VMEM((size, units, rows, v, 2 * v), BF16),
                pltpu.VMEM((units, size * rows, v, 2 * v), BF16),
                pltpu.VMEM((o * SUB, size * rows * SUB), BF16),
                pltpu.VMEM((o, v, 2 * v), F32),
                pltpu.VMEM((o, v, 2 * v), F32),
                pltpu.VMEM((o, 2 * v), F32),
                pltpu.SemaphoreType.DMA((slots,)),
                pltpu.SemaphoreType.DMA((parts,)),
                pltpu.SemaphoreType.DMA((4,)),
                pltpu.SemaphoreType.DMA,
                pltpu.SemaphoreType.DMA((2 + len(groups) - joint,)),
            ],
            compiler_params=pltpu.CompilerParams(collective_id=0, has_side_effects=True, vmem_limit_bytes=62 * 2**20),
        )(a_ints, c_occ.T, c_vir.T, eps_occ.reshape(1, o), eps_vir.reshape(1, v)).T

    return jax.shard_map(
        per_device,
        mesh=mesh,
        in_specs=(P(("frag", "dev")), P("frag"), P("frag"), P("frag"), P("frag")),
        out_specs=P("frag", "dev"),
        check_vma=False,
    )
```

```python
import functools

import jax
import jax.numpy as jnp
from jax import lax
from jax.experimental import pallas as pl
from jax.experimental.pallas import tpu as pltpu
from jax.sharding import PartitionSpec as P

MESH = pl.DeviceIdType.MESH
LANES = 128
SUB = 16
F32, BF16 = jnp.float32, jnp.bfloat16


def dot(lhs, rhs):
    return jnp.dot(lhs, rhs, preferred_element_type=F32)


def iota(shape, dim):
    return lax.broadcasted_iota(jnp.int32, shape, dim)


def one_hot(mask):
    return mask.astype(F32).astype(BF16)


def kernel(dims, a_hbm, cot_hbm, cvt_hbm, eo_hbm, ev_hbm, out_ref, abuf, cot, cvt, eo, ev, lhs, wv, tbuf, hbuf, gsend, grecv, kron, vbuf, wbuf, ebuf,
           a_sem, first_sem, c_sem, send_sem, recv_sem):
    rows, n, o, v, size, slots, units, groups, joint, parts = dims
    me, frag = lax.axis_index("dev"), lax.axis_index("frag")
    chips = size // 2
    chip, core = me // 2, me % 2
    pair = 2 * v
    od = o // size
    total = size * rows
    starts = [sum(groups[:g]) for g in range(len(groups))]
    last = len(groups) - 1

    def peer(dx, dc):
        return lax.rem(chip + dx, chips) * 2 + lax.rem(core + dc, 2)

    relations = [(dx, dc) for dx in sorted(range(chips), key=lambda d: -min(d, chips - d)) for dc in range(2) if (dx, dc) != (0, 0)]

    def load(p):
        slot = lax.rem(p, slots)
        return pltpu.make_async_copy(a_hbm.at[p], abuf.at[slot], a_sem.at[slot])

    small = [pltpu.make_async_copy(src, dst, c_sem.at[k]) for k, (src, dst) in enumerate([(cot_hbm, cot), (cvt_hbm, cvt), (eo_hbm, eo), (ev_hbm, ev)])]
    cuts = [0, n * 9 // 16 // 2 * 2, n]
    opening = [pltpu.make_async_copy(a_hbm.at[0, pl.ds(x, y - x)], abuf.at[0, pl.ds(x, y - x)], first_sem.at[k])
               for k, (x, y) in enumerate(zip(cuts, cuts[1:]))]
    small[0].start()
    small[1].start()
    for copy in opening:
        copy.start()
    barrier = pltpu.get_barrier_semaphore()
    for dx, dc in relations:
        pl.semaphore_signal(barrier, inc=1, device_id=(frag, peer(dx, dc)), device_id_type=MESH)

    with jax.named_scope("waitC"):
        small[0].wait()
        small[1].wait()
    for p in range(1, min(slots, rows)):
        load(p).start()
    small[2].start()
    small[3].start()
    row, col = iota((o, o), 0), iota((o, o), 1)
    lhs[...] = dot(one_hot(col == lax.rem(row, size) * od + row // (2 * size) * 2 + lax.rem(row // size, 2)), cot[...]).astype(BF16)
    cv = jnp.pad(cvt[...].astype(F32), ((0, 0), (0, LANES - n))).T.astype(BF16)
    zero = jnp.zeros_like(cv)
    wv[...] = jnp.concatenate([jnp.concatenate([cv, zero], 1), jnp.concatenate([zero, cv], 1)], 0)

    def share(which, group, rel, sem):
        start, count = starts[group], groups[group]
        target = peer(*relations[rel])
        return pltpu.make_async_remote_copy(
            src_ref=gsend.at[target, which, pl.ds(start, count)],
            dst_ref=grecv.at[which, pl.ds(size * start + me * count, count)],
            send_sem=send_sem,
            recv_sem=recv_sem.at[sem],
            device_id=(frag, target),
            device_id_type=MESH,
        )

    def arrivals(which, count, sem):
        part = grecv.at[which, pl.ds(0, (size - 1) * count)]
        return pltpu.make_async_remote_copy(
            src_ref=part, dst_ref=part, send_sem=send_sem, recv_sem=recv_sem.at[sem], device_id=(frag, peer(*relations[0])), device_id_type=MESH)

    every, first_unit, other_units = pl.ds(0, units), pl.ds(0, 1), pl.ds(1, units - 1)

    def send(which, group, sem):
        for rel in range(len(relations)):
            share(which, group, rel, sem).start()

    def occupied(slot, first, end):
        fill = jnp.zeros((n, LANES - n), BF16)
        for q in range(first, end, 2):
            t = dot(lhs[...], jnp.concatenate([abuf[slot, q], fill, abuf[slot, q + 1], fill], 1))
            tbuf[pl.ds(q, o, stride=n), :] = t[:, :LANES]
            tbuf[pl.ds(q + 1, o, stride=n), :] = t[:, LANES:]

    depth = size * n

    def half_mo(unit, first, end):
        even, odd = (tbuf[(2 * unit + k) * depth + first:(2 * unit + k) * depth + end, :] for k in range(2))
        return dot(jnp.concatenate([even, odd], 1).astype(BF16), wv[...])

    def virtual(unit, p):
        with jax.named_scope("step3"):
            for d in range(0, size, 2):
                h = jnp.concatenate([hbuf[unit * depth + k * n:unit * depth + (k + 1) * n, :] for k in (d, d + 1)], 1)
                g = dot(cvt[...], h.astype(BF16)).astype(BF16)
                for k in range(2):
                    gsend[d + k, unit, p] = g[:, k * pair:(k + 1) * pair]

    def open_row():
        for k, copy in enumerate(opening):
            with jax.named_scope("waitA"):
                copy.wait()
            with jax.named_scope("step1"):
                occupied(0, cuts[k], cuts[k + 1])
        if slots < rows:
            load(slots).start()
        for unit in range(units):
            with jax.named_scope("step2"):
                for k in range(2):
                    at = k * depth // 2
                    hbuf[unit * depth + at:unit * depth + at + depth // 2, :] = half_mo(unit, at, at + depth // 2)
            virtual(unit, 0)
            if unit == 0:
                with jax.named_scope("waitB"):
                    pl.semaphore_wait(barrier, len(relations))
            send(pl.ds(unit, 1), 0, 0)

    def next_row(p, carry):
        slot = lax.rem(p, slots)
        with jax.named_scope("waitA"):
            load(p).wait()
        with jax.named_scope("step1"):
            occupied(slot, 0, n)

        @pl.when(p + slots < rows)
        def _():
            load(p + slots).start()

        with jax.named_scope("step2"):
            for unit in range(units):
                hbuf[unit * depth:(unit + 1) * depth, :] = half_mo(unit, 0, depth)
        for unit in range(units):
            virtual(unit, p)
        for group in range(1, len(groups)):
            @pl.when(p == starts[group] + groups[group] - 1)
            def _(group=group):
                if group < joint:
                    send(every, group, 0)
                else:
                    send(first_unit, group, 1)
        return carry

    open_row()
    lax.fori_loop(1, rows, next_row, 0)
    for group in range(joint, len(groups)):
        send(other_units, group, 2 + group - joint)

    small[2].wait()
    small[3].wait()
    with jax.named_scope("kron"):
        by_p = dot(one_hot(iota((o * SUB, o), 0) // SUB == iota((o * SUB, o), 1)), cot[...]).astype(BF16)
        for start, count in zip(starts, groups):
            for at in range(size * start * SUB, size * (start + count) * SUB, 2 * LANES):
                width = min(2 * LANES, size * (start + count) * SUB - at)
                place = (iota((total, width), 1) + at) // SUB - size * start
                spread_p = one_hot(iota((total, width), 0) == place // count * rows + start + place % count)
                same = iota((o * SUB, width), 0) % SUB == iota((o * SUB, width), 1) % SUB
                kron[:, at:at + width] = jnp.where(same, dot(by_p, spread_p), 0.0).astype(BF16)

    for unit in range(units):
        for start, count in zip(starts, groups):
            grecv[unit, pl.ds(size * start + me * count, count)] = gsend[me, unit, start:start + count]

    ev_row, eo_row = ev[...], eo[...]
    diag = iota((v, v), 0) == iota((v, v), 1)
    ev_col = jnp.sum(jnp.where(diag, jnp.broadcast_to(ev_row, (v, v)), 0.0), 1, keepdims=True)
    eo_col = jnp.sum(jnp.where(row == col, jnp.broadcast_to(eo_row, (o, o)), 0.0), 1, keepdims=True)
    left = iota((v, pair), 1) < v

    def weights(unit):
        with jax.named_scope("W"):
            energy_j = [jnp.sum(jnp.where(iota((1, o), 1) == me * od + 2 * unit + h, eo_row, 0.0), 1, keepdims=True) for h in range(2)]
            base = jnp.concatenate([e - ev_row for e in energy_j], 1) - ev_col
            for i in range(o):
                wbuf[i] = 1.0 / (eo_col[i:i + 1, :] + base)

    def integrals(unit, first, end, add):
        with jax.named_scope("V"):
            width = (end - first) * SUB
            for block in range(0, v, 2 * SUB):
                rhs = jnp.concatenate([grecv[unit, first:end, block + k * SUB:block + (k + 1) * SUB, :].reshape(width, pair) for k in range(2)], 1)
                part = dot(kron[:, first * SUB:end * SUB], rhs)
                for k in range(2):
                    at = slice(block + k * SUB, block + (k + 1) * SUB)
                    new = part[:, k * pair:(k + 1) * pair].reshape(o, SUB, pair)
                    vbuf[:, at, :] = vbuf[:, at, :] + new if add else new

    def energies():
        with jax.named_scope("E"):
            for i in range(0, o, 2):
                x = vbuf[i:i + 2].reshape(2 * v, pair)
                xt = x.T
                turned = pltpu.roll(jnp.where(left, xt[v:], xt[:v]), v, 1)
                top = jnp.where(left, xt[:v], turned)
                bottom = jnp.where(left, turned, xt[v:])
                for k, swap in enumerate((top, bottom)):
                    own = x[k * v:(k + 1) * v]
                    ebuf[i + k:i + k + 1, :] = jnp.sum(own * (2.0 * own - swap) * wbuf[i + k], 0, keepdims=True)

    def totals():
        with jax.named_scope("sum"):
            sums = ebuf[...].T
            return [jnp.sum(sums[h * v:(h + 1) * v], 0, keepdims=True) for h in range(2)]

    pairs = []
    for unit in range(units):
        weights(unit)
        if unit == 0:
            with jax.named_scope("waitR"):
                arrivals(every, starts[joint], 0).wait_recv()
                arrivals(first_unit, rows - starts[joint], 1).wait_recv()
            integrals(unit, 0, total, False)
        else:
            for group in range(joint, len(groups)):
                if unit == 1:
                    with jax.named_scope(f"waitR{group}"):
                        arrivals(other_units, groups[group], 2 + group - joint).wait_recv()
                first = group == joint
                integrals(unit, 0 if first else size * starts[group], size * (starts[group] + groups[group]), not first)
        energies()
        pairs += totals()
    out_ref[...] = jnp.concatenate(pairs, 0)

    sent = gsend.at[pl.ds(0, size - 1)]
    with jax.named_scope("waitS"):
        pltpu.make_async_remote_copy(
            src_ref=sent, dst_ref=sent, send_sem=send_sem, recv_sem=recv_sem.at[0], device_id=(frag, peer(*relations[0])), device_id_type=MESH).wait_send()


def solution(mesh):
    size = mesh.shape["dev"]

    def per_device(a_ints, c_occ, c_vir, eps_occ, eps_vir):
        rows, n = a_ints.shape[0], a_ints.shape[1]
        o, v = c_occ.shape[1], c_vir.shape[1]
        units = o // size // 2
        slots, parts = 4, 2
        groups = (1, 1, 2, rows - 8, 2, 2)
        joint = 3
        dims = (rows, n, o, v, size, slots, units, groups, joint, parts)
        any_spec = pl.BlockSpec(memory_space=pl.ANY)
        return pl.pallas_call(
            functools.partial(kernel, dims),
            out_shape=pltpu.VMEM((o // size, o), F32),
            in_specs=[any_spec] * 5,
            out_specs=pl.BlockSpec(memory_space=pltpu.VMEM),
            scratch_shapes=[
                pltpu.VMEM((slots, n, n, n), BF16),
                pltpu.VMEM((o, n), BF16),
                pltpu.VMEM((v, n), BF16),
                pltpu.VMEM((1, o), F32),
                pltpu.VMEM((1, v), F32),
                pltpu.VMEM((o, n), BF16),
                pltpu.VMEM((2 * LANES, 2 * v), BF16),
                pltpu.VMEM((o * n, LANES), F32),
                pltpu.VMEM((units * size * n, 2 * v), F32),
                pltpu.VMEM((size, units, rows, v, 2 * v), BF16),
                pltpu.VMEM((units, size * rows, v, 2 * v), BF16),
                pltpu.VMEM((o * SUB, size * rows * SUB), BF16),
                pltpu.VMEM((o, v, 2 * v), F32),
                pltpu.VMEM((o, v, 2 * v), F32),
                pltpu.VMEM((o, 2 * v), F32),
                pltpu.SemaphoreType.DMA((slots,)),
                pltpu.SemaphoreType.DMA((parts,)),
                pltpu.SemaphoreType.DMA((4,)),
                pltpu.SemaphoreType.DMA,
                pltpu.SemaphoreType.DMA((2 + len(groups) - joint,)),
            ],
            compiler_params=pltpu.CompilerParams(collective_id=0, has_side_effects=True, vmem_limit_bytes=62 * 2**20),
        )(a_ints, c_occ.T, c_vir.T, eps_occ.reshape(1, o), eps_vir.reshape(1, v)).T

    return jax.shard_map(
        per_device,
        mesh=mesh,
        in_specs=(P(("frag", "dev")), P("frag"), P("frag"), P("frag"), P("frag")),
        out_specs=P("frag", "dev"),
        check_vma=False,
    )
```

```python
import functools

import jax
import jax.numpy as jnp
from jax import lax
from jax.experimental import pallas as pl
from jax.experimental.pallas import tpu as pltpu
from jax.sharding import PartitionSpec as P

MESH = pl.DeviceIdType.MESH
LANES = 128
SUB = 16
F32, BF16 = jnp.float32, jnp.bfloat16


def dot(lhs, rhs):
    return jnp.dot(lhs, rhs, preferred_element_type=F32)


def iota(shape, dim):
    return lax.broadcasted_iota(jnp.int32, shape, dim)


def one_hot(mask):
    return mask.astype(F32).astype(BF16)


def kernel(dims, a_hbm, cot_hbm, cvt_hbm, eo_hbm, ev_hbm, out_ref, abuf, cot, cvt, eo, ev, lhs, wv, tbuf, hbuf, gsend, grecv, kron, vbuf, wbuf, ebuf,
           a_sem, first_sem, c_sem, send_sem, recv_sem):
    rows, n, o, v, size, slots, units, groups, joint, parts = dims
    me, frag = lax.axis_index("dev"), lax.axis_index("frag")
    chips = size // 2
    chip, core = me // 2, me % 2
    pair = 2 * v
    od = o // size
    total = size * rows
    starts = [sum(groups[:g]) for g in range(len(groups))]
    last = len(groups) - 1

    def peer(dx, dc):
        return lax.rem(chip + dx, chips) * 2 + lax.rem(core + dc, 2)

    relations = [(dx, dc) for dx in sorted(range(chips), key=lambda d: -min(d, chips - d)) for dc in range(2) if (dx, dc) != (0, 0)]

    def load(p):
        slot = lax.rem(p, slots)
        return pltpu.make_async_copy(a_hbm.at[p], abuf.at[slot], a_sem.at[slot])

    small = [pltpu.make_async_copy(src, dst, c_sem.at[k]) for k, (src, dst) in enumerate([(cot_hbm, cot), (cvt_hbm, cvt), (eo_hbm, eo), (ev_hbm, ev)])]
    cuts = [0, n * 9 // 16 // 2 * 2, n]
    opening = [pltpu.make_async_copy(a_hbm.at[0, pl.ds(x, y - x)], abuf.at[0, pl.ds(x, y - x)], first_sem.at[k])
               for k, (x, y) in enumerate(zip(cuts, cuts[1:]))]
    small[0].start()
    small[1].start()
    for copy in opening:
        copy.start()
    barrier = pltpu.get_barrier_semaphore()
    for dx, dc in relations:
        pl.semaphore_signal(barrier, inc=1, device_id=(frag, peer(dx, dc)), device_id_type=MESH)

    with jax.named_scope("waitC"):
        small[0].wait()
        small[1].wait()
    for p in range(1, min(slots, rows)):
        load(p).start()
    small[2].start()
    small[3].start()
    row, col = iota((o, o), 0), iota((o, o), 1)
    lhs[...] = dot(one_hot(col == lax.rem(row, size) * od + row // (2 * size) * 2 + lax.rem(row // size, 2)), cot[...]).astype(BF16)
    cv = jnp.pad(cvt[...].astype(F32), ((0, 0), (0, LANES - n))).T.astype(BF16)
    zero = jnp.zeros_like(cv)
    wv[...] = jnp.concatenate([jnp.concatenate([cv, zero], 1), jnp.concatenate([zero, cv], 1)], 0)

    def share(which, group, rel, sem):
        start, count = starts[group], groups[group]
        target = peer(*relations[rel])
        return pltpu.make_async_remote_copy(
            src_ref=gsend.at[target, which, pl.ds(start, count)],
            dst_ref=grecv.at[which, pl.ds(size * start + me * count, count)],
            send_sem=send_sem,
            recv_sem=recv_sem.at[sem],
            device_id=(frag, target),
            device_id_type=MESH,
        )

    def arrivals(which, count, sem):
        part = grecv.at[which, pl.ds(0, (size - 1) * count)]
        return pltpu.make_async_remote_copy(
            src_ref=part, dst_ref=part, send_sem=send_sem, recv_sem=recv_sem.at[sem], device_id=(frag, peer(*relations[0])), device_id_type=MESH)

    every, first_unit, other_units = pl.ds(0, units), pl.ds(0, 1), pl.ds(1, units - 1)

    def send(which, group, sem):
        for rel in range(len(relations)):
            share(which, group, rel, sem).start()

    def occupied(slot, first, end):
        fill = jnp.zeros((n, LANES - n), BF16)
        for q in range(first, end, 2):
            t = dot(lhs[...], jnp.concatenate([abuf[slot, q], fill, abuf[slot, q + 1], fill], 1))
            tbuf[pl.ds(q, o, stride=n), :] = t[:, :LANES]
            tbuf[pl.ds(q + 1, o, stride=n), :] = t[:, LANES:]

    depth = size * n

    def half_mo(unit, first, end):
        even, odd = (tbuf[(2 * unit + k) * depth + first:(2 * unit + k) * depth + end, :] for k in range(2))
        return dot(jnp.concatenate([even, odd], 1).astype(BF16), wv[...])

    def virtual(unit, p):
        with jax.named_scope("step3"):
            for d in range(0, size, 2):
                h = jnp.concatenate([hbuf[unit * depth + k * n:unit * depth + (k + 1) * n, :] for k in (d, d + 1)], 1)
                g = dot(cvt[...], h.astype(BF16)).astype(BF16)
                for k in range(2):
                    gsend[d + k, unit, p] = g[:, k * pair:(k + 1) * pair]

    def open_row():
        for k, copy in enumerate(opening):
            with jax.named_scope("waitA"):
                copy.wait()
            with jax.named_scope("step1"):
                occupied(0, cuts[k], cuts[k + 1])
        if slots < rows:
            load(slots).start()
        for unit in range(units):
            with jax.named_scope("step2"):
                for k in range(2):
                    at = k * depth // 2
                    hbuf[unit * depth + at:unit * depth + at + depth // 2, :] = half_mo(unit, at, at + depth // 2)
            virtual(unit, 0)
            if unit == 0:
                with jax.named_scope("waitB"):
                    pl.semaphore_wait(barrier, len(relations))
            send(pl.ds(unit, 1), 0, 0)

    def next_row(p, carry):
        slot = lax.rem(p, slots)
        with jax.named_scope("waitA"):
            load(p).wait()
        with jax.named_scope("step1"):
            occupied(slot, 0, n)

        @pl.when(p + slots < rows)
        def _():
            load(p + slots).start()

        with jax.named_scope("step2"):
            for unit in range(units):
                hbuf[unit * depth:(unit + 1) * depth, :] = half_mo(unit, 0, depth)
        for unit in range(units):
            virtual(unit, p)
        for group in range(1, len(groups)):
            @pl.when(p == starts[group] + groups[group] - 1)
            def _(group=group):
                if group < joint:
                    send(every, group, 0)
                else:
                    send(first_unit, group, 1)
        return carry

    open_row()
    lax.fori_loop(1, rows, next_row, 0)
    for group in range(joint, len(groups)):
        send(other_units, group, 2 + group - joint)

    small[2].wait()
    small[3].wait()
    with jax.named_scope("kron"):
        by_p = dot(one_hot(iota((o * SUB, o), 0) // SUB == iota((o * SUB, o), 1)), cot[...]).astype(BF16)
        for start, count in zip(starts, groups):
            for at in range(size * start * SUB, size * (start + count) * SUB, 2 * LANES):
                width = min(2 * LANES, size * (start + count) * SUB - at)
                place = (iota((total, width), 1) + at) // SUB - size * start
                spread_p = one_hot(iota((total, width), 0) == place // count * rows + start + place % count)
                same = iota((o * SUB, width), 0) % SUB == iota((o * SUB, width), 1) % SUB
                kron[:, at:at + width] = jnp.where(same, dot(by_p, spread_p), 0.0).astype(BF16)

    for unit in range(units):
        for start, count in zip(starts, groups):
            grecv[unit, pl.ds(size * start + me * count, count)] = gsend[me, unit, start:start + count]

    ev_row, eo_row = ev[...], eo[...]
    diag = iota((v, v), 0) == iota((v, v), 1)
    ev_col = jnp.sum(jnp.where(diag, jnp.broadcast_to(ev_row, (v, v)), 0.0), 1, keepdims=True)
    eo_col = jnp.sum(jnp.where(row == col, jnp.broadcast_to(eo_row, (o, o)), 0.0), 1, keepdims=True)
    left = iota((v, pair), 1) < v

    def weights(unit):
        with jax.named_scope("W"):
            energy_j = [jnp.sum(jnp.where(iota((1, o), 1) == me * od + 2 * unit + h, eo_row, 0.0), 1, keepdims=True) for h in range(2)]
            base = jnp.concatenate([e - ev_row for e in energy_j], 1) - ev_col
            for i in range(o):
                wbuf[i] = 1.0 / (eo_col[i:i + 1, :] + base)

    def integrals(unit, first, end, add):
        with jax.named_scope("V"):
            width = (end - first) * SUB
            for block in range(0, v, 2 * SUB):
                rhs = jnp.concatenate([grecv[unit, first:end, block + k * SUB:block + (k + 1) * SUB, :].reshape(width, pair) for k in range(2)], 1)
                part = dot(kron[:, first * SUB:end * SUB], rhs)
                for k in range(2):
                    at = slice(block + k * SUB, block + (k + 1) * SUB)
                    new = part[:, k * pair:(k + 1) * pair].reshape(o, SUB, pair)
                    vbuf[:, at, :] = vbuf[:, at, :] + new if add else new

    def energies():
        with jax.named_scope("E"):
            for i in range(0, o, 2):
                x = vbuf[i:i + 2].reshape(2 * v, pair)
                xt = x.T
                turned = pltpu.roll(jnp.where(left, xt[v:], xt[:v]), v, 1)
                top = jnp.where(left, xt[:v], turned)
                bottom = jnp.where(left, turned, xt[v:])
                for k, swap in enumerate((top, bottom)):
                    own = x[k * v:(k + 1) * v]
                    ebuf[i + k:i + k + 1, :] = jnp.sum(own * (2.0 * own - swap) * wbuf[i + k], 0, keepdims=True)

    def totals():
        with jax.named_scope("sum"):
            sums = ebuf[...].T
            return [jnp.sum(sums[h * v:(h + 1) * v], 0, keepdims=True) for h in range(2)]

    pairs = []
    for unit in range(units):
        weights(unit)
        if unit == 0:
            with jax.named_scope("waitR"):
                arrivals(every, starts[joint], 0).wait_recv()
                arrivals(first_unit, rows - starts[joint], 1).wait_recv()
            integrals(unit, 0, total, False)
        else:
            for group in range(joint, len(groups)):
                if unit == 1:
                    with jax.named_scope(f"waitR{group}"):
                        arrivals(other_units, groups[group], 2 + group - joint).wait_recv()
                first = group == joint
                integrals(unit, 0 if first else size * starts[group], size * (starts[group] + groups[group]), not first)
        energies()
        pairs += totals()
    out_ref[...] = jnp.concatenate(pairs, 0)

    sent = gsend.at[pl.ds(0, size - 1)]
    with jax.named_scope("waitS"):
        pltpu.make_async_remote_copy(
            src_ref=sent, dst_ref=sent, send_sem=send_sem, recv_sem=recv_sem.at[0], device_id=(frag, peer(*relations[0])), device_id_type=MESH).wait_send()


def solution(mesh):
    size = mesh.shape["dev"]

    def per_device(a_ints, c_occ, c_vir, eps_occ, eps_vir):
        rows, n = a_ints.shape[0], a_ints.shape[1]
        o, v = c_occ.shape[1], c_vir.shape[1]
        units = o // size // 2
        slots, parts = 4, 2
        groups = (1, 1, 2, rows - 8, 2, 2)
        joint = 4
        dims = (rows, n, o, v, size, slots, units, groups, joint, parts)
        any_spec = pl.BlockSpec(memory_space=pl.ANY)
        return pl.pallas_call(
            functools.partial(kernel, dims),
            out_shape=pltpu.VMEM((o // size, o), F32),
            in_specs=[any_spec] * 5,
            out_specs=pl.BlockSpec(memory_space=pltpu.VMEM),
            scratch_shapes=[
                pltpu.VMEM((slots, n, n, n), BF16),
                pltpu.VMEM((o, n), BF16),
                pltpu.VMEM((v, n), BF16),
                pltpu.VMEM((1, o), F32),
                pltpu.VMEM((1, v), F32),
                pltpu.VMEM((o, n), BF16),
                pltpu.VMEM((2 * LANES, 2 * v), BF16),
                pltpu.VMEM((o * n, LANES), F32),
                pltpu.VMEM((units * size * n, 2 * v), F32),
                pltpu.VMEM((size, units, rows, v, 2 * v), BF16),
                pltpu.VMEM((units, size * rows, v, 2 * v), BF16),
                pltpu.VMEM((o * SUB, size * rows * SUB), BF16),
                pltpu.VMEM((o, v, 2 * v), F32),
                pltpu.VMEM((o, v, 2 * v), F32),
                pltpu.VMEM((o, 2 * v), F32),
                pltpu.SemaphoreType.DMA((slots,)),
                pltpu.SemaphoreType.DMA((parts,)),
                pltpu.SemaphoreType.DMA((4,)),
                pltpu.SemaphoreType.DMA,
                pltpu.SemaphoreType.DMA((2 + len(groups) - joint,)),
            ],
            compiler_params=pltpu.CompilerParams(collective_id=0, has_side_effects=True, vmem_limit_bytes=62 * 2**20),
        )(a_ints, c_occ.T, c_vir.T, eps_occ.reshape(1, o), eps_vir.reshape(1, v)).T

    return jax.shard_map(
        per_device,
        mesh=mesh,
        in_specs=(P(("frag", "dev")), P("frag"), P("frag"), P("frag"), P("frag")),
        out_specs=P("frag", "dev"),
        check_vma=False,
    )
```
